256 devices in a mesh: leaf: 256 (over z, x, y, core).
Axes of the slice: x: 4, y: 4, z: 8, core: 2. Of those that a mesh axis runs over, the one named last changes fastest.
Arguments:
- right_sides: bfloat16 [32, 524288], P(None, 'leaf'), may hold values from -6 to 6
- point_order: int32 [256, 2048], P('leaf'), may hold values from 0 to 2047, each once within a row
- leaf_inverse: bfloat16 [524288, 2048], P('leaf'), may hold values from -0.09375 to 0.09375
- basis_in: bfloat16 [524288, 256], P('leaf'), may hold values from -0.125 to 0.125
- basis_out: bfloat16 [65536, 2048], P('leaf'), may hold values from -0.1875 to 0.1875
- leaf_up: bfloat16 [65536, 256], P('leaf'), may hold values from -0.25 to 0.25
- leaf_down: bfloat16 [65536, 256], P('leaf'), may hold values from -0.3125 to 0.3125
- node_up: bfloat16 [65536, 256], P('leaf'), may hold values from -0.25 to 0.25
- node_down: bfloat16 [65536, 256], P('leaf'), may hold values from -0.3125 to 0.3125
- node_cross: bfloat16 [131072, 256], P('leaf'), may hold values from -0.25 to 0.25
- leaf_map: int32 [256], replicated, may hold values from 0 to 255, as said below
Outputs:
- solution: float32 [32, 524288], P(None, 'leaf')
The draws below stay inside these ranges and needn't reach their ends.
Inputs may be any that keep to these rules, and one draw needn't show every extreme that they name: `point_order`: each row is a permutation of the leaf's columns. `leaf_map`: A permutation of the tree positions that keeps every device's leaf inside the device's aligned block of 4 devices.
All inputs are finite; a program needn't handle non-finite values.
Results may differ from the reference program's by a relative error of at most 0.015.
Values may be sent and summed in bfloat16 or wider, within the bound.
A program may use at most 192 MiB of HBM per device.

```python
import jax
import jax.numpy as jnp
from jax import lax

LEAF = 2048
RANK = 256
RHS = 32
SPREAD = 4
LEAVES = 256
POINTS = 524288
N_LEAF = 256


def draw_leaf_map(key, part):
    groups = LEAVES // SPREAD
    keys = jax.random.split(jax.random.fold_in(key, 7), groups)
    local = jax.vmap(lambda single: jax.random.permutation(single, SPREAD))(keys)
    offsets = (jnp.arange(groups, dtype=jnp.int32) * SPREAD)[:, None]
    return (local.astype(jnp.int32) + offsets).reshape(LEAVES).astype(jnp.int32)


def shard_levels(key, dims, cuts, least, high):
    gain = 1.0
    for dim, parts in cuts:
        heights = jax.random.uniform(jax.random.fold_in(jax.random.fold_in(key, 6), dim), (parts,), jnp.float32, least / len(cuts), high / len(cuts))
        gain = gain * jnp.repeat(jnp.exp(heights), dims[dim] // parts).reshape((-1,) + (1,) * (len(dims) - 1 - dim))
    return gain


def scatter_about(own_key, extent, scale, bound, pieces=(), kind=jnp.bfloat16):
    array = scale * jax.random.normal(own_key, extent, jnp.float32)
    if pieces:
        array = array * shard_levels(own_key, extent, pieces, -0.22, 0.18)
    return jnp.clip(array, -bound, bound).astype(kind)


def setup_inputs(seed: int = 0) -> dict:
    arg_keys = jax.random.split(jax.random.key(seed), 12)
    return {
        "right_sides": scatter_about(arg_keys[0], (RHS, POINTS), 1.0, 6.0, ((1, 256),)),
        "point_order": jax.vmap(lambda own: jax.random.permutation(own, LEAF))(jax.random.split(arg_keys[1], LEAVES)).reshape((LEAVES, LEAF)).astype(jnp.int32),
        "leaf_inverse": scatter_about(arg_keys[2], (POINTS, LEAF), (2 * LEAF) ** -0.5, 0.09375, ((0, 256),)),
        "basis_in": scatter_about(arg_keys[3], (POINTS, RANK), LEAF ** -0.5, 0.125, ((0, 256),)),
        "basis_out": scatter_about(arg_keys[4], (LEAVES * RANK, LEAF), (4 * RANK) ** -0.5, 0.1875, ((0, 256),)),
        "leaf_up": scatter_about(arg_keys[5], (LEAVES * RANK, RANK), (2 * RANK) ** -0.5, 0.25, ((0, 256),)),
        "leaf_down": scatter_about(arg_keys[6], (LEAVES * RANK, RANK), (4 * RANK // 3) ** -0.5, 0.3125, ((0, 256),)),
        "node_up": scatter_about(arg_keys[7], (LEAVES * RANK, RANK), (2 * RANK) ** -0.5, 0.25, ((0, 256),)),
        "node_down": scatter_about(arg_keys[8], (LEAVES * RANK, RANK), (4 * RANK // 3) ** -0.5, 0.3125, ((0, 256),)),
        "node_cross": scatter_about(arg_keys[9], (LEAVES * 2 * RANK, RANK), (2 * RANK) ** -0.5, 0.25, ((0, 256),)),
        "leaf_map": draw_leaf_map(jax.random.fold_in(arg_keys[11], 71), 0),
    }


def reference(right_sides, point_order, leaf_inverse, basis_in, basis_out, leaf_up, leaf_down, node_up, node_down, node_cross, leaf_map):
    members = N_LEAF
    levels = members.bit_length() - 1
    blocks = jnp.transpose(right_sides.reshape(RHS, members, LEAF), (1, 0, 2))
    tree_rhs = jnp.take_along_axis(blocks, point_order[:, None, :], axis=2)
    inverses = leaf_inverse.reshape(members, LEAF, LEAF)
    inward = basis_in.reshape(members, LEAF, RANK)
    outward = basis_out.reshape(members, RANK, LEAF)

    def leaf_terms(items):
        segment, inverse, basis = items
        near = jnp.dot(segment, inverse, preferred_element_type=jnp.float32)
        coarse = jnp.dot(segment, basis, preferred_element_type=jnp.float32).astype(jnp.bfloat16)
        return near, coarse

    near_terms, reduced = lax.map(leaf_terms, (tree_rhs, inverses, inward))
    source = jnp.zeros((members,), jnp.int32).at[leaf_map].set(jnp.arange(members, dtype=jnp.int32))
    current = reduced[source]
    leaf_ups = leaf_up.reshape(members, RANK, RANK).astype(jnp.float32)
    leaf_downs = leaf_down.reshape(members, RANK, RANK).astype(jnp.float32)
    node_ups = node_up.reshape(members, RANK, RANK).astype(jnp.float32)
    node_downs = node_down.reshape(members, RANK, RANK).astype(jnp.float32)
    couplings = node_cross.reshape(members, 2, RANK, RANK).astype(jnp.float32)
    stored = []
    for height in range(1, levels + 1):
        children = members >> (height - 1)
        if height == 1:
            up_maps = leaf_ups
        else:
            owners = (1 << (height - 1)) * jnp.arange(children) + (1 << (height - 2))
            up_maps = node_ups[owners]
        product = jnp.einsum("nab,nbc->nac", current.astype(jnp.float32), up_maps)
        stored.append((current[0::2], current[1::2]))
        current = (product[0::2] + product[1::2]).astype(jnp.bfloat16)
    top_map = node_up.reshape(members, RANK, RANK)[members // 2]
    node_f = jnp.dot(current[0], top_map, preferred_element_type=jnp.float32).astype(jnp.bfloat16)[None]
    for height in range(levels, 0, -1):
        left_g, right_g = stored[height - 1]
        parents = members >> height
        owners = (1 << height) * jnp.arange(parents) + (1 << (height - 1))
        pair = couplings[owners]
        if height == 1:
            down_maps = leaf_downs
        else:
            child_owners = (1 << (height - 1)) * jnp.arange(2 * parents) + (1 << (height - 2))
            down_maps = node_downs[child_owners]
        parent_f = node_f.astype(jnp.float32)
        left_f = jnp.einsum("nab,nbc->nac", right_g.astype(jnp.float32), pair[:, 0]) + jnp.einsum("nab,nbc->nac", parent_f, down_maps[0::2])
        right_f = jnp.einsum("nab,nbc->nac", left_g.astype(jnp.float32), pair[:, 1]) + jnp.einsum("nab,nbc->nac", parent_f, down_maps[1::2])
        node_f = jnp.stack([left_f.astype(jnp.bfloat16), right_f.astype(jnp.bfloat16)], 1).reshape(2 * parents, RHS, RANK)
    leaf_f = node_f[leaf_map]

    def finish(items):
        near, coarse, basis, ordering = items
        answer = near + jnp.dot(coarse, basis, preferred_element_type=jnp.float32)
        return jnp.zeros_like(answer).at[:, ordering].set(answer)

    placed = lax.map(finish, (near_terms, leaf_f, outward, point_order))
    return jnp.transpose(placed, (1, 0, 2)).reshape(RHS, members * LEAF)
```

```python
import jax
import jax.numpy as jnp
import numpy as np
from jax import lax
from jax.experimental import pallas as pl
from jax.experimental.pallas import tpu as pltpu
from jax.sharding import PartitionSpec as P

MESH = pl.DeviceIdType.MESH
BF = jnp.bfloat16
F32 = jnp.float32
TILE = 256

SLOTS = (
    "W1", "R1", "B1", "W2", "V2", "R2", "B2", "B3", "W3", "R3", "W4", "R4", "B4", "B5",
    "W5", "R5", "W6", "R6", "B6", "R7", "B7", "W7", "V7", "S", "B8",
)
SLOT = {name: i for i, name in enumerate(SLOTS)}


def div(value, by):
    return lax.div(value, np.int32(by))


def rem(value, by):
    return lax.rem(value, np.int32(by))


def bit(value, i):
    return rem(div(value, 1 << i), 2)


def flip(value, mask):
    out = value
    for i in range(8):
        if mask >> i & 1:
            out = out + (1 - 2 * bit(value, i)) * (1 << i)
    return out


def mm(a, b):
    return jnp.dot(a, b, preferred_element_type=F32)


def kernel(
    rs_hbm, order_hbm, inv_hbm, vin_hbm, uout_hbm, lup_hbm, ldn_hbm,
    nup_hbm, ndn_hbm, ncr_hbm, lmap_hbm,
    out_ref,
    rs, order, inv, vin, lhs, sel, tree, uperm, nperm, fin,
    lmap, w0, r0, mats, comp, compx, route, ysend, yin, y2in,
    xsend, xin, x5in, zsend, zin, z7in, f5in, f3in, rex, cex,
    local_sem, send_sem, recv_sem,
):
    me = lax.axis_index("leaf")
    rank = w0.shape[0]
    points = rs.shape[1]
    rows = rs.shape[0]
    tiles = points // TILE

    is_y = rem(me, 8) == 1
    is_x = rem(me, 32) == 1
    level = [None] + [rem(me, 1 << k) == 1 << (k - 1) for k in range(1, 9)]
    ycen = div(me, 8) * 8 + 1
    xcen = div(me, 32) * 32 + 1
    ypos = rem(me, 8)
    xpos = rem(div(me, 8), 4)
    half = div(me, 128)
    neighbour = flip(me, 1)

    barrier = pltpu.get_barrier_semaphore()

    def greet(target):
        pl.semaphore_signal(barrier, inc=1, device_id=(target,), device_id_type=MESH)

    for r in range(1, 8):
        greet(flip(me, r))

    own4 = div(me, 16) * 16 + 8
    own5 = div(me, 32) * 32 + 16
    own6 = div(me, 64) * 64 + 32

    @pl.when(is_y)
    def _():
        for r in range(1, 4):
            greet(flip(me, 8 * r))
        greet(own4)
        greet(own5)

    @pl.when(is_x)
    def _():
        for r in range(1, 8):
            greet(flip(me, 32 * r))
        greet(own6)
        greet(64)
        greet(192)
        greet(128)

    def fetch(src, dst, i):
        return pltpu.make_async_copy(src, dst, local_sem.at[i])

    loads = [
        fetch(order_hbm, order, 0),
        fetch(rs_hbm, rs, 1),
        fetch(vin_hbm, vin, 2),
        fetch(lmap_hbm, lmap, 3),
        fetch(lup_hbm, w0, 4),
        fetch(inv_hbm, inv, 5),
        fetch(uout_hbm, lhs.at[pl.ds(0, rank)], 6),
        fetch(ldn_hbm, r0, 7),
    ]
    for load in loads:
        load.start()

    counter = [0]
    sent = {}

    def slot_of(name):
        return mats.at[SLOT[name]]

    n_mats = len(SLOTS)
    recv_at = {}
    base = n_mats
    for name, count in (
        ("route", 4), ("yin", 8), ("y2in", 8), ("xin", 4), ("x5in", 4),
        ("zin", 8), ("z7in", 8), ("f5in", 1), ("f3in", 1), ("rex", 4), ("cex", 4),
    ):
        recv_at[name] = base
        base += count

    def send(role, src, dst, rsem, target):
        i = counter[0]
        counter[0] += 1
        pltpu.make_async_remote_copy(
            src_ref=src, dst_ref=dst, send_sem=send_sem.at[i], recv_sem=recv_sem.at[rsem],
            device_id=(target,), device_id_type=MESH,
        ).start()
        sent.setdefault(role, []).append((i, dst.shape[0] == rank))

    def arrived(dst, rsem):
        pltpu.make_async_remote_copy(
            src_ref=dst, dst_ref=dst, send_sem=send_sem.at[0], recv_sem=recv_sem.at[rsem],
            device_id=(neighbour,), device_id_type=MESH,
        ).wait_recv()

    def need(*names):
        for name in names:
            arrived(slot_of(name), SLOT[name])

    def ship(role, name, src, target):
        send(role, src, slot_of(name), SLOT[name], target)

    def keep(name, src):
        pltpu.make_async_copy(src, slot_of(name), recv_sem.at[SLOT[name]]).start()

    left = ncr_hbm.at[pl.ds(0, rank)]
    right = ncr_hbm.at[pl.ds(rank, rank)]

    loads[0].wait()
    loads[1].wait()

    def gather(t, carry):
        cols = pl.ds(pl.multiple_of(t * TILE, TILE), TILE)
        ids = lax.broadcasted_iota(jnp.int32, (points, TILE), 0)
        hot = jnp.where(ids == order[:, cols], 1.0, 0.0).astype(BF)
        sel[:, cols] = hot
        tree[:, cols] = mm(rs[...], hot).astype(BF)
        return carry

    lax.fori_loop(0, tiles, gather, 0)

    n_in = (
        7
        + jnp.where(is_y, 3, 0)
        + jnp.where(is_x, 7, 0)
        + jnp.where(level[4], 2, 0)
        + jnp.where(level[5], 4, 0)
        + jnp.where(level[6], 2, 0)
        + jnp.where(level[7], 8, 0)
        + jnp.where(level[8], 8, 0)
    )
    pl.semaphore_wait(barrier, n_in)

    left2 = rem(me, 8) == 2
    right2 = rem(me, 8) == 6

    @pl.when(left2)
    def _():
        ship("L2l", "W2", nup_hbm, me - 1)

    @pl.when(right2)
    def _():
        ship("L2r", "V2", nup_hbm, me - 5)

    @pl.when(level[1])
    def _():
        ship("L1", "W1", nup_hbm, me - 1)
        keep("W1", nup_hbm)

    @pl.when(level[3])
    def _():
        ship("L3", "W3", nup_hbm, me - 3)

    @pl.when(level[4])
    def _():
        for target, side in ((me - 7, left), (me + 1, right)):
            ship("L4", "W4", nup_hbm, target)
            ship("L4", "R4", ndn_hbm, target)
            ship("L4", "B4", side, target)

    @pl.when(level[5])
    def _():
        ship("L5", "W5", nup_hbm, me - 15)
        ship("L5", "R5", ndn_hbm, me - 15)
        for i in range(4):
            ship("L5", "B5", left if i < 2 else right, me - 15 + 8 * i)

    @pl.when(level[6])
    def _():
        for i in range(2):
            ship("L6", "W6", nup_hbm, me - 31 + 32 * i)
        for i in range(2):
            ship("L6", "R6", ndn_hbm, me - 31 + 32 * i)
            ship("L6", "B6", left if i < 1 else right, me - 31 + 32 * i)

    @pl.when(level[7])
    def _():
        for i in range(4):
            ship("L7", "V7", nup_hbm, (1 - half) * 128 + 1 + 32 * i)
        for i in range(4):
            target = half * 128 + 1 + 32 * i
            ship("L7", "R7", ndn_hbm, target)
            ship("L7", "W7", nup_hbm, target)
            ship("L7", "B7", left if i < 2 else right, target)

    @pl.when(level[8])
    def _():
        for i in (0, 7, 1, 6, 2, 5, 3, 4):
            target = 1 + 32 * i
            ship("L8", "S", nup_hbm, target)
            ship("L8", "B8", left if i < 4 else right, target)

    loads[2].wait()
    route[0] = mm(tree[...], vin[...]).astype(BF)
    for r in (3, 2, 1):
        send("all", route.at[0], route.at[r], recv_at["route"] + r, flip(me, r))

    @pl.when(level[1])
    def _():
        ship("L1", "R1", ndn_hbm, me - 1)
        keep("R1", ndn_hbm)
        ship("L1", "B1", left, me - 1)
        keep("B1", right)

    loads[4].wait()
    need("W1")
    comp[0] = mm(w0[...], slot_of("W1")[...]).astype(BF)

    loads[3].wait()
    source = np.int32(0)
    for r in range(1, 4):
        source = jnp.where(lmap[flip(me, r)] == me, r, source)
    for r in range(1, 4):
        arrived(route.at[r], recv_at["route"] + r)
    g0 = route[source]
    ysend[0] = g0
    ysend[2] = mm(g0, comp[0]).astype(BF)

    @pl.when(jnp.logical_not(is_y))
    def _():
        send("notY", ysend.at[2], y2in.at[ypos], recv_at["y2in"] + ypos, ycen)

    ysend[1] = mm(g0, w0[...]).astype(BF)
    for r in (7, 6, 5, 4, 3, 2, 1):
        k = 2 if r >= 4 else 1 if r >= 2 else 0
        send("all", ysend.at[k], yin.at[r], recv_at["yin"] + r, flip(me, r))

    @pl.when(level[2])
    def _():
        keep("R2", ndn_hbm)
        keep("B2", right)
        for r in (3, 2, 1):
            ship("L2", "R2", ndn_hbm, flip(me, r))
            ship("L2", "B2", right if r == 1 else left, flip(me, r))

    @pl.when(level[3])
    def _():
        ship("L3", "R3", ndn_hbm, me - 3)
        for i in range(8):
            src = left if i < 4 else right
            if i == 4:
                keep("B3", src)
            else:
                ship("L3", "B3", src, me + (i - 4))

    loads[5].wait()

    def near(t, carry):
        cols = pl.ds(pl.multiple_of(t * TILE, TILE), TILE)
        value = mm(tree[...], inv[:, cols])
        high = value.astype(BF)
        lhs[pl.ds(rank, rows), cols] = high
        lhs[pl.ds(rank + rows, rows), cols] = (value - high.astype(F32)).astype(BF)
        return carry

    lax.fori_loop(0, tiles, near, 0)

    @pl.when(is_y)
    def _():
        need("W3", "W4")
        compx[0] = mm(slot_of("W3")[...], slot_of("W4")[...]).astype(BF)
        need("W2", "V2")
        total = ysend[2].astype(F32)
        for i in (0, 2, 3):
            arrived(y2in.at[i], recv_at["y2in"] + i)
            total = total + y2in[i].astype(F32)
        g3 = mm(total.astype(BF), slot_of("W2")[...])
        for i in (4, 5, 6, 7):
            arrived(y2in.at[i], recv_at["y2in"] + i)
        total = (
            y2in[4].astype(F32) + y2in[5].astype(F32) + y2in[6].astype(F32) + y2in[7].astype(F32)
        )
        g3 = (g3 + mm(total.astype(BF), slot_of("V2")[...])).astype(BF)
        xsend[0] = g3
        xsend[2] = mm(g3, compx[0]).astype(BF)

        @pl.when(jnp.logical_not(is_x))
        def _():
            send("YnotX", xsend.at[2], x5in.at[xpos], recv_at["x5in"] + xpos, xcen)

        xsend[1] = mm(g3, slot_of("W3")[...]).astype(BF)
        for r in (3, 2, 1):
            send("Y", xsend.at[1 if r >= 2 else 0], xin.at[r], recv_at["xin"] + r, flip(me, 8 * r))

    loads[6].wait()

    def scatter(t, carry):
        cols = pl.ds(pl.multiple_of(t * TILE, TILE), TILE)
        both = lax.dot_general(
            lhs[...], sel[cols, :], (((1,), (1,)), ((), ())), preferred_element_type=F32
        )
        uperm[:, cols] = both[:rank].astype(BF)
        nperm[:, cols] = both[rank : rank + rows] + both[rank + rows :]
        return carry

    lax.fori_loop(0, tiles, scatter, 0)

    @pl.when(is_x)
    def _():
        need("W5", "W6")
        compx[1] = mm(slot_of("W5")[...], slot_of("W6")[...]).astype(BF)
        total = xsend[2].astype(F32)
        for s in range(1, 4):
            arrived(x5in.at[s], recv_at["x5in"] + s)
            total = total + x5in[s].astype(F32)
        g5 = total.astype(BF)
        zsend[0] = g5
        zsend[2] = mm(g5, compx[1]).astype(BF)
        for r in (4, 5, 6, 7, 3, 2, 1):
            send("X", zsend.at[2], z7in.at[r], recv_at["z7in"] + r, flip(me, 32 * r))
        zsend[1] = mm(g5, slot_of("W5")[...]).astype(BF)
        for r in (3, 2, 1):
            send("X", zsend.at[1 if r >= 2 else 0], zin.at[r], recv_at["zin"] + r, flip(me, 32 * r))

    loads[7].wait()
    need("R1")
    comp[0] = mm(slot_of("R1")[...], r0[...]).astype(BF)
    need("R2")
    rex[0] = mm(slot_of("R2")[...], comp[0]).astype(BF)
    for r in (3, 2, 1):
        send("all", rex.at[0], rex.at[r], recv_at["rex"] + r, flip(me, r))
    for r in range(1, 8):
        arrived(yin.at[r], recv_at["yin"] + r)
    need("B3", "B2", "B1")
    g2 = yin[4].astype(F32) + yin[5].astype(F32) + yin[6].astype(F32) + yin[7].astype(F32)
    g1 = yin[2].astype(F32) + yin[3].astype(F32)
    part = mm(g2.astype(BF), slot_of("B3")[...]).astype(BF)
    part = (mm(g1.astype(BF), slot_of("B2")[...]) + mm(part, slot_of("R1")[...])).astype(BF)
    cex[0] = (mm(yin[1], slot_of("B1")[...]) + mm(part, r0[...])).astype(BF)
    for r in (3, 2, 1):
        send("all", cex.at[0], cex.at[r], recv_at["cex"] + r, flip(me, r))

    @pl.when(is_y)
    def _():
        need("R3", "R4", "B4", "B5")
        compx[2] = mm(slot_of("R4")[...], slot_of("R3")[...]).astype(BF)
        for r in range(1, 4):
            arrived(xin.at[r], recv_at["xin"] + r)
        g4 = (xin[2].astype(F32) + xin[3].astype(F32)).astype(BF)
        upper = mm(g4, slot_of("B5")[...]).astype(BF)
        fin[:, pl.ds(0, rank)] = mm(xin[1], slot_of("B4")[...]) + mm(upper, slot_of("R3")[...])

    @pl.when(is_x)
    def _():
        need("R5", "R6", "B6", "B7", "R7", "S", "W7", "V7", "B8")
        r65 = mm(slot_of("R6")[...], slot_of("R5")[...]).astype(BF)
        compx[3] = mm(slot_of("B7")[...], slot_of("R5")[...]).astype(BF)
        top = mm(slot_of("S")[...], slot_of("R7")[...]).astype(BF)
        top = mm(top, r65).astype(BF)
        compx[4] = mm(slot_of("W7")[...], top).astype(BF)
        compx[5] = (mm(slot_of("V7")[...], top) + mm(slot_of("B8")[...], r65)).astype(BF)
        for r in range(1, 4):
            arrived(zin.at[r], recv_at["zin"] + r)
        g6 = (zin[2].astype(F32) + zin[3].astype(F32)).astype(BF)
        value = mm(zin[1], slot_of("B6")[...]) + mm(g6, compx[3])
        g7 = zsend[2].astype(F32)
        for r in range(1, 4):
            arrived(z7in.at[r], recv_at["z7in"] + r)
            g7 = g7 + z7in[r].astype(F32)
        value = value + mm(g7.astype(BF), compx[4])
        for r in range(4, 8):
            arrived(z7in.at[r], recv_at["z7in"] + r)
        g7 = (
            z7in[4].astype(F32) + z7in[5].astype(F32) + z7in[6].astype(F32) + z7in[7].astype(F32)
        )
        value = value + mm(g7.astype(BF), compx[5])
        f5in[...] = value.astype(BF)
        for r in (2, 3, 1):
            send("X", f5in, f5in, recv_at["f5in"], flip(me, 8 * r))

    @pl.when(is_y)
    def _():
        @pl.when(jnp.logical_not(is_x))
        def _():
            arrived(f5in, recv_at["f5in"])

        f3in[...] = (mm(f5in[...], compx[2]) + fin[:, pl.ds(0, rank)]).astype(BF)
        for r in (5, 4, 7, 6, 3, 2, 1):
            send("Y", f3in, f3in, recv_at["f3in"], flip(me, r))

    for r in range(1, 4):
        arrived(rex.at[r], recv_at["rex"] + r)
    for r in range(1, 4):
        arrived(cex.at[r], recv_at["cex"] + r)
    place = lmap[me]
    pick = np.int32(0)
    for r in range(1, 4):
        pick = jnp.where(place == flip(me, r), r, pick)
    down = rex[pick]
    cross = cex[pick]

    def close(t, carry):
        cols = pl.ds(pl.multiple_of(t * TILE, TILE), TILE)
        nperm[:, cols] = nperm[:, cols] + mm(cross, uperm[:, cols])
        uperm[:, cols] = mm(down, uperm[:, cols]).astype(BF)
        return carry

    lax.fori_loop(0, tiles, close, 0)

    @pl.when(jnp.logical_not(is_y))
    def _():
        arrived(f3in, recv_at["f3in"])

    out_ref[...] = nperm[...] + mm(f3in[...], uperm[...])

    def drain(role):
        for i, is_square in sent.get(role, []):
            like = mats.at[0] if is_square else route.at[0]
            pltpu.make_async_remote_copy(
                src_ref=like, dst_ref=like, send_sem=send_sem.at[i], recv_sem=recv_sem.at[0],
                device_id=(neighbour,), device_id_type=MESH,
            ).wait_send()

    drain("all")
    for role, cond in (
        ("notY", jnp.logical_not(is_y)),
        ("YnotX", jnp.logical_and(is_y, jnp.logical_not(is_x))),
        ("Y", is_y), ("X", is_x),
        ("L1", level[1]), ("L2l", left2), ("L2r", right2), ("L2", level[2]), ("L3", level[3]), ("L4", level[4]),
        ("L5", level[5]), ("L6", level[6]), ("L7", level[7]), ("L8", level[8]),
    ):
        @pl.when(cond)
        def _(role=role):
            drain(role)

    assert counter[0] <= send_sem.shape[0], counter[0]
    assert base <= recv_sem.shape[0], base


def solution(mesh):
    def body(
        right_sides, point_order, leaf_inverse, basis_in, basis_out, leaf_up, leaf_down,
        node_up, node_down, node_cross, leaf_map,
    ):
        rows, points = right_sides.shape
        rank = leaf_up.shape[0]
        small = (rows, rank)
        square = (rank, rank)
        anywhere = pl.BlockSpec(memory_space=pl.ANY)
        return pl.pallas_call(
            kernel,
            out_shape=pltpu.VMEM((rows, points), F32),
            in_specs=[anywhere] * 11,
            out_specs=pl.BlockSpec(memory_space=pltpu.VMEM),
            scratch_shapes=[
                pltpu.VMEM((rows, points), BF),
                pltpu.VMEM((1, points), jnp.int32),
                pltpu.VMEM((points, points), BF),
                pltpu.VMEM((points, rank), BF),
                pltpu.VMEM((rank + 2 * rows, points), BF),
                pltpu.VMEM((points, points), BF),
                pltpu.VMEM((rows, points), BF),
                pltpu.VMEM((rank, points), BF),
                pltpu.VMEM((rows, points), F32),
                pltpu.VMEM(small, F32),
                pltpu.SMEM(leaf_map.shape, jnp.int32),
                pltpu.VMEM(square, BF),
                pltpu.VMEM(square, BF),
                pltpu.VMEM((len(SLOTS),) + square, BF),
                pltpu.VMEM((2,) + square, BF),
                pltpu.VMEM((6,) + square, BF),
                pltpu.VMEM((4,) + small, BF),
                pltpu.VMEM((4,) + small, BF),
                pltpu.VMEM((8,) + small, BF),
                pltpu.VMEM((8,) + small, BF),
                pltpu.VMEM((3,) + small, BF),
                pltpu.VMEM((4,) + small, BF),
                pltpu.VMEM((4,) + small, BF),
                pltpu.VMEM((3,) + small, BF),
                pltpu.VMEM((8,) + small, BF),
                pltpu.VMEM((8,) + small, BF),
                pltpu.VMEM(small, BF),
                pltpu.VMEM(small, BF),
                pltpu.VMEM((4,) + square, BF),
                pltpu.VMEM((4,) + small, BF),
                pltpu.SemaphoreType.DMA((8,)),
                pltpu.SemaphoreType.DMA((128,)),
                pltpu.SemaphoreType.DMA((80,)),
            ],
            compiler_params=pltpu.CompilerParams(
                collective_id=0, has_side_effects=True, vmem_limit_bytes=56 * 1024 * 1024
            ),
        )(
            right_sides, point_order, leaf_inverse, basis_in, basis_out, leaf_up, leaf_down,
            node_up, node_down, node_cross, leaf_map,
        )

    placed = (P(None, "leaf"),) + (P("leaf", None),) * 9 + (P(),)
    return jax.shard_map(
        body, mesh=mesh, in_specs=placed, out_specs=P(None, "leaf"), check_vma=False
    )
```
